32 devices in a mesh: grp: 4 (over y, x), dev: 8 (over z, core).
Axes of the slice: x: 2, y: 2, z: 4, core: 2. Of those that a mesh axis runs over, the one named last changes fastest.
Arguments:
- leaf_emit: float32 [3, 4096], P(None, 'dev'), may hold values from 0 to 1
- leaf_albedo: float32 [3, 4096], P(None, 'dev'), may hold values from 0.2 to 0.9
- leaf_radiosity: float32 [3, 4096], P(None, 'dev'), may hold values from 0.05 to 4
- leaf_area: float32 [4096], P('dev'), may hold values from 0.002 to 0.03
- parent_index: int32 [4096], P('dev'), may hold values from 0 to 255, as said below
- node_position: float32 [3, 6144], P(None, 'dev'), may hold values from -1 to 1
- node_angles: float32 [2, 6144], P(None, 'dev'), may hold values from -3.140625 to 3.140625
- block_receiver: int32 [4, 1024], P('grp', 'dev'), may hold values from 0 to 5
- block_source: int32 [4, 1024], P('grp', 'dev'), may hold values from 0 to 15
- block_count: int32 [4, 8], P('grp', 'dev'), may hold values from 16 to 128, as said below
Outputs:
- new_radiosity: float32 [3, 4096], P(None, 'dev')
The draws below stay inside these ranges and needn't reach their ends.
Inputs may be any that keep to these rules, and one draw needn't show every extreme that they name: `parent_index`: within each shard's 512 leaves every cluster 0 to 255 is named at least once. The first block_count slots of a device are live, the rest are ignored. For every index of dev exactly one index of grp has 128 live slots; the others have at most 64.
All inputs are finite; a program needn't handle non-finite values.
Results may differ from the reference program's by a relative error of at most 0.0001.
Values sent between devices are 32-bit elements; how exact they have to be, the bound alone decides.
A program may use at most 64 MiB of HBM per device.

```python
import math
import jax
import jax.numpy as jnp
from jax import lax

TILE = 128
LEAF_DEV = 512
PAR_DEV = 256
BLK = 128
GROUPS = 4
SHARDS = 8
NODE_DEV = 768
NT = 6
SRC_TILES = 16
LEAVES = 4096
NODES = 6144


def draw_parent_index(key, part):
    shard_count = LEAVES // LEAF_DEV
    shard_keys = jax.random.split(key, shard_count)

    def one_shard(shard_key):
        first_key, second_key = jax.random.split(shard_key)
        covered = jnp.arange(PAR_DEV, dtype=jnp.int32)
        others = jax.random.randint(first_key, (LEAF_DEV - PAR_DEV,), 0, PAR_DEV, dtype=jnp.int32)
        return jax.random.permutation(second_key, jnp.concatenate([covered, others]))
    return jax.vmap(one_shard)(shard_keys).reshape(LEAVES).astype(jnp.int32)


def draw_block_count(key, part):
    first_key, second_key = jax.random.split(jax.random.fold_in(key, 7))
    counts = jax.random.randint(first_key, (GROUPS, SHARDS), BLK // 8, BLK // 2 + 1, dtype=jnp.int32)
    heavy = jax.random.randint(second_key, (SHARDS,), 0, GROUPS, dtype=jnp.int32)
    group_rows = jnp.arange(GROUPS, dtype=jnp.int32)[:, None]
    return jnp.where(group_rows == heavy[None, :], BLK, counts).astype(jnp.int32)


def set_ends(entries, rng, least, high):
    longest = entries.shape.index(max(entries.shape))
    spots = []
    for shift in (0, 1):
        where = [jax.random.randint(jax.random.fold_in(rng, axis), (), 0, length) for axis, length in enumerate(entries.shape)]
        where[longest] = (where[longest] + shift) % entries.shape[longest]
        spots.append(tuple(where))
    return entries.at[spots[0]].set(least).at[spots[1]].set(high)


def steps_of(stream_key, extent, pieces, low, high):
    factor_of, own = 1.0, jax.random.fold_in(stream_key, 6)
    for position, shards_of in pieces:
        draws = jnp.exp(jax.random.uniform(jax.random.fold_in(own, position), (shards_of,), jnp.float32, low / len(pieces), high / len(pieces)))
        factor_of = factor_of * jnp.repeat(draws, extent[position] // shards_of).reshape([-1 if axis == position else 1 for axis in range(len(extent))])
    return factor_of


def setup_inputs(seed: int = 0) -> dict:
    key_list = jax.random.split(jax.random.key(seed), 11)
    leaf_emit = jnp.clip(1.0 * jax.random.uniform(key_list[0], (3, LEAVES), jnp.float32) ** steps_of(key_list[0], (3, LEAVES), ((1, 8),), -0.2, 0.2), 0.0, 1.0)
    leaf_albedo = jnp.clip(0.2 + 0.7 * jax.random.uniform(key_list[1], (3, LEAVES), jnp.float32) ** steps_of(key_list[1], (3, LEAVES), ((1, 8),), -0.2, 0.2), 0.2, 0.9)
    leaf_radiosity = jnp.clip(jnp.exp(math.log(4.0) - 4.3820266 * jax.random.uniform(key_list[2], (3, LEAVES), jnp.float32) ** steps_of(key_list[2], (3, LEAVES), ((1, 8),), -0.2, 0.2)), 0.05, 4.0)
    leaf_area = jnp.clip(jnp.exp(math.log(0.03) - 2.70805 * jax.random.uniform(key_list[3], (LEAVES,), jnp.float32) ** steps_of(key_list[3], (LEAVES,), ((0, 8),), -0.2, 0.2)), 0.002, 0.03)
    parent_index = draw_parent_index(jax.random.fold_in(key_list[10], 71), 0)
    node_position = jnp.clip(jax.random.uniform(key_list[5], (3, NODES), jnp.float32, -1.0, 1.0) * steps_of(key_list[5], (3, NODES), ((1, 8),), -0.4, 0.0), -1.0, 1.0)
    node_angles = jnp.clip(jax.random.uniform(key_list[6], (2, NODES), jnp.float32, -3.140625, 3.140625), -3.140625, 3.140625)
    block_receiver = set_ends(jax.random.randint(key_list[7], (GROUPS, SHARDS * BLK), 0, NT), jax.random.fold_in(key_list[7], 1), 0, NT - 1).astype(jnp.int32)
    block_source = set_ends(jax.random.randint(key_list[8], (GROUPS, SHARDS * BLK), 0, SRC_TILES), jax.random.fold_in(key_list[8], 1), 0, SRC_TILES - 1).astype(jnp.int32)
    block_count = draw_block_count(jax.random.fold_in(key_list[10], 71), 0)
    return {"leaf_emit": leaf_emit, "leaf_albedo": leaf_albedo, "leaf_radiosity": leaf_radiosity, "leaf_area": leaf_area, "parent_index": parent_index, "node_position": node_position, "node_angles": node_angles, "block_receiver": block_receiver, "block_source": block_source, "block_count": block_count}


def unit_normals(node_angles):
    azimuth = node_angles[0]
    elevation = node_angles[1]
    return jnp.stack([jnp.cos(azimuth) * jnp.cos(elevation), jnp.sin(azimuth) * jnp.cos(elevation), jnp.sin(elevation)])


def tile_irradiance(receivers, sources):
    offsets = [sources[axis_id][:, None, :] - receivers[axis_id][:, :, None] for axis_id in range(3)]
    distance_sq = offsets[0] * offsets[0] + offsets[1] * offsets[1] + offsets[2] * offsets[2]
    facing_receiver = receivers[3][:, :, None] * offsets[0] + receivers[4][:, :, None] * offsets[1] + receivers[5][:, :, None] * offsets[2]
    facing_source = sources[3][:, None, :] * offsets[0] + sources[4][:, None, :] * offsets[1] + sources[5][:, None, :] * offsets[2]
    source_area = sources[6][:, None, :]
    factor = source_area * jnp.maximum(facing_receiver, 0.0) * jnp.maximum(-facing_source, 0.0) / ((distance_sq + source_area) * (jnp.pi * distance_sq + source_area))
    return jnp.einsum('bij,cbj->bci', factor, sources[7:10], precision=lax.Precision.HIGHEST)


def reference(leaf_emit, leaf_albedo, leaf_radiosity, leaf_area, parent_index, node_position, node_angles, block_receiver, block_source, block_count):
    shard_count = SHARDS
    per_peer = NODE_DEV // shard_count
    normals = unit_normals(node_angles)
    positions = node_position.reshape(3, shard_count, NODE_DEV)
    normals = normals.reshape(3, shard_count, NODE_DEV)
    patch_area = leaf_area.reshape(shard_count, LEAF_DEV)
    radiosity = leaf_radiosity.reshape(3, shard_count, LEAF_DEV)
    parents = parent_index.reshape(shard_count, LEAF_DEV)
    parent_onehot = (parents[:, :, None] == jnp.arange(PAR_DEV, dtype=jnp.int32)[None, None, :]).astype(jnp.float32)
    cluster_area = jnp.einsum('sl,slp->sp', patch_area, parent_onehot, precision=lax.Precision.HIGHEST)
    weighted = jnp.einsum('csl,slp->csp', radiosity * patch_area[None], parent_onehot, precision=lax.Precision.HIGHEST)
    cluster_radiosity = weighted / cluster_area[None]
    source_pack = jnp.concatenate([positions[:, :, LEAF_DEV:], normals[:, :, LEAF_DEV:], cluster_area[None], cluster_radiosity], axis=0)
    source_tiles = source_pack.reshape(10, SRC_TILES, TILE)
    receiver_octree = jnp.concatenate([positions, normals], axis=0)
    receiver_link = receiver_octree.reshape(6, shard_count, shard_count, per_peer).transpose(0, 2, 1, 3)
    receiver_tiles = receiver_link.reshape(6, shard_count * NT, TILE)
    tile_offset = (jnp.arange(shard_count, dtype=jnp.int32) * NT)[None, :, None]
    receiver_ids = (block_receiver.reshape(GROUPS, shard_count, BLK) + tile_offset).reshape(GROUPS * shard_count, BLK)
    source_ids = block_source.reshape(GROUPS * shard_count, BLK)
    live_weight = (jnp.arange(BLK, dtype=jnp.int32)[None, None, :] < block_count[:, :, None]).astype(jnp.float32)
    live_weight = live_weight.reshape(GROUPS * shard_count, BLK)

    def accumulate(totals, batch):
        batch_receivers, batch_sources, batch_weight = batch
        receivers = jnp.take(receiver_tiles, batch_receivers, axis=1)
        sources = jnp.take(source_tiles, batch_sources, axis=1)
        contrib = tile_irradiance(receivers, sources) * batch_weight[:, None, None]
        return totals.at[batch_receivers].add(contrib), None

    initial = jnp.zeros((shard_count * NT, 3, TILE), jnp.float32)
    totals, unused = lax.scan(accumulate, initial, (receiver_ids, source_ids, live_weight))
    link_order = totals.reshape(shard_count, NT, 3, TILE).transpose(2, 0, 1, 3).reshape(3, shard_count, NODE_DEV)
    octree_order = link_order.reshape(3, shard_count, shard_count, per_peer).transpose(0, 2, 1, 3).reshape(3, shard_count, NODE_DEV)
    pushed = jnp.einsum('csp,slp->csl', octree_order[:, :, LEAF_DEV:], parent_onehot, precision=lax.Precision.HIGHEST)
    gathered = octree_order[:, :, :LEAF_DEV] + pushed
    return leaf_emit + leaf_albedo * gathered.reshape(3, shard_count * LEAF_DEV)
```

```python
import functools
import jax
import jax.numpy as jnp
from jax import lax
from jax.experimental import pallas as pl
from jax.experimental.pallas import tpu as pltpu
from jax.sharding import PartitionSpec as P

TILE = 128


batch_slots = 16


def unit_normals(node_angles):
    azimuth = node_angles[0]
    elevation = node_angles[1]
    return jnp.stack(
        [
            jnp.cos(azimuth) * jnp.cos(elevation),
            jnp.sin(azimuth) * jnp.cos(elevation),
            jnp.sin(elevation),
        ]
    )


def tile_irradiance(receivers, sources):
    offsets = [
        sources[axis_id][:, None, :] - receivers[axis_id][:, :, None] for axis_id in range(3)
    ]
    distance_sq = offsets[0] * offsets[0] + offsets[1] * offsets[1] + offsets[2] * offsets[2]
    facing_receiver = (
        receivers[3][:, :, None] * offsets[0]
        + receivers[4][:, :, None] * offsets[1]
        + receivers[5][:, :, None] * offsets[2]
    )
    facing_source = (
        sources[3][:, None, :] * offsets[0]
        + sources[4][:, None, :] * offsets[1]
        + sources[5][:, None, :] * offsets[2]
    )
    source_area = sources[6][:, None, :]
    factor = (
        source_area
        * jnp.maximum(facing_receiver, 0.0)
        * jnp.maximum(-facing_source, 0.0)
        / ((distance_sq + source_area) * (jnp.pi * distance_sq + source_area))
    )
    return jnp.einsum("bij,cbj->bci", factor, sources[7:10], precision=lax.Precision.HIGHEST)


def listed_body(
    leaf_emit,
    leaf_albedo,
    leaf_radiosity,
    leaf_area,
    parent_index,
    node_position,
    node_angles,
    block_receiver,
    block_source,
    block_count,
):
    leaf_count = leaf_area.shape[0]
    node_count = node_position.shape[1]
    cluster_count = node_count - leaf_count
    tile_count = node_count // TILE
    slot_count = block_receiver.shape[1]
    normals = unit_normals(node_angles)
    parent_onehot = (
        parent_index[:, None] == jnp.arange(cluster_count, dtype=jnp.int32)[None, :]
    ).astype(jnp.float32)
    cluster_area = jnp.dot(leaf_area, parent_onehot, precision=lax.Precision.HIGHEST)
    weighted = jnp.dot(
        leaf_radiosity * leaf_area[None, :], parent_onehot, precision=lax.Precision.HIGHEST
    )
    cluster_radiosity = weighted / cluster_area[None, :]
    source_pack = jnp.concatenate(
        [
            node_position[:, leaf_count:],
            normals[:, leaf_count:],
            cluster_area[None, :],
            cluster_radiosity,
        ],
        axis=0,
    )
    receiver_pack = jnp.concatenate([node_position, normals], axis=0)
    linked = lax.all_to_all(receiver_pack, "dev", split_axis=1, concat_axis=1, tiled=True)
    receiver_tiles = linked.reshape(6, tile_count, TILE)
    everything = lax.all_gather(source_pack, "dev", axis=1, tiled=True)
    source_tiles = everything.reshape(10, -1, TILE)
    receiver_ids = block_receiver[0]
    source_ids = block_source[0]
    live_count = block_count[0, 0]
    step_slots = min(batch_slots, slot_count)

    def add_batch(rounds, totals):
        first = rounds * step_slots
        batch_receivers = lax.dynamic_slice_in_dim(receiver_ids, first, step_slots, 0)
        batch_sources = lax.dynamic_slice_in_dim(source_ids, first, step_slots, 0)
        batch_weight = (first + jnp.arange(step_slots, dtype=jnp.int32) < live_count).astype(
            jnp.float32
        )
        receivers = jnp.take(receiver_tiles, batch_receivers, axis=1)
        sources = jnp.take(source_tiles, batch_sources, axis=1)
        contrib = tile_irradiance(receivers, sources) * batch_weight[:, None, None]
        placement = (
            batch_receivers[:, None] == jnp.arange(tile_count, dtype=jnp.int32)[None, :]
        ).astype(jnp.float32)
        return totals + jnp.einsum(
            "bt,bci->cti", placement, contrib, precision=lax.Precision.HIGHEST
        )

    batch_total = (live_count + step_slots - 1) // step_slots
    totals = lax.fori_loop(0, batch_total, add_batch, jnp.zeros((3, tile_count, TILE), jnp.float32))
    partial_value = totals.reshape(3, node_count)
    summed = lax.psum(partial_value, "grp")
    irradiance = lax.all_to_all(summed, "dev", split_axis=1, concat_axis=1, tiled=True)
    pushed = jnp.dot(irradiance[:, leaf_count:], parent_onehot.T, precision=lax.Precision.HIGHEST)
    gathered = irradiance[:, :leaf_count] + pushed
    return leaf_emit + leaf_albedo * gathered


F32 = jnp.float32
BF16 = jnp.bfloat16
MESH = pl.DeviceIdType.MESH
ROWS = 10
NT_DIMS = (((1,), (1,)), ((), ()))


def split3(values):
    high = values.astype(BF16)
    rest = values - high.astype(F32)
    middle = rest.astype(BF16)
    low = (rest - middle.astype(F32)).astype(BF16)
    return [high.astype(F32), middle.astype(F32), low.astype(F32)]


def stack3(values):
    rows = values.shape[0]
    pad = jnp.zeros((16 - 3 * rows, values.shape[1]), F32)
    return jnp.concatenate(split3(values) + [pad], axis=0).astype(BF16)


def unstack3(product, rows):
    return product[0:rows] + product[rows : 2 * rows] + product[2 * rows : 3 * rows]


def dense_kernel(
    groups, shards, radiosity, area, parent, position, angles, receiver_id, source_id, count,
    out, packs, sources, columns, my_hist, hists, receivers, onehot, place, sums, part, gathered,
    src_send, src_recv, hist_send, hist_recv, part_send, part_recv,
):
    g = lax.axis_index("grp")
    k = lax.axis_index("dev")
    device_total = groups * shards
    me = g * shards + k
    leaves = radiosity.shape[1]
    nodes = position.shape[1]
    clusters = nodes - leaves
    per_shard = clusters // TILE
    source_tiles = shards * per_shard
    tiles_here = source_tiles // groups
    per_peer = nodes // shards
    chunks = nodes // TILE

    barrier = pltpu.get_barrier_semaphore()

    def greet(step, carry):
        other = (me + step) % device_total
        pl.semaphore_signal(
            barrier, inc=1, device_id=(other // shards, other % shards), device_id_type=MESH
        )
        return carry

    lax.fori_loop(1, device_total, greet, 0)

    lane = lax.broadcasted_iota(jnp.int32, (1, TILE), 1)
    code = receiver_id[...] * source_tiles + source_id[...]
    code = jnp.where(lane < count[0, 0], code, -1)
    square = lax.broadcasted_iota(jnp.int32, (TILE, TILE), 0)
    hit = jnp.where(square == code, 1.0, 0.0).astype(BF16)
    counted = lax.dot_general(
        jnp.ones((16, TILE), BF16), hit, NT_DIMS, preferred_element_type=F32
    )
    my_hist[...] = counted[0:1]
    hists[me] = counted[0:1]

    ids = lax.broadcasted_iota(jnp.int32, (clusters, leaves), 0)
    onehot[...] = jnp.where(ids == parent[...], 1.0, 0.0).astype(BF16)
    area_row = area[...]
    stacked = stack3(jnp.concatenate([area_row, radiosity[...] * area_row], axis=0))
    cluster = unstack3(
        lax.dot_general(stacked, onehot[...], NT_DIMS, preferred_element_type=F32), 4
    )
    cosines = jnp.cos(angles[...])
    sines = jnp.sin(angles[...])
    normals = [cosines[0:1] * cosines[1:2], sines[0:1] * cosines[1:2], sines[1:2]]
    node_rows = [position[i : i + 1, :] for i in range(3)] + normals
    for half in range(per_shard):
        first = leaves + half * TILE
        rows = [row[:, first : first + TILE] for row in node_rows]
        rows.append(cluster[:, half * TILE : (half + 1) * TILE])
        packs[half] = jnp.concatenate(rows, axis=0)

    half = (g + groups * shards * per_shard - per_shard * k) % groups
    is_owner = half < per_shard
    mine = (per_shard * k + half) // groups

    pl.semaphore_wait(barrier, device_total - 1)

    def source_copy(step):
        return pltpu.make_async_remote_copy(
            src_ref=packs.at[half],
            dst_ref=sources.at[mine],
            send_sem=src_send.at[step - 1],
            recv_sem=src_recv.at[mine],
            device_id=(g, (k + step) % shards),
            device_id_type=MESH,
        )

    @pl.when(is_owner)
    def _():
        for step in range(1, shards):
            source_copy(step).start()
        sources[mine] = packs[half]

    def send_hist(step, carry):
        other = (me + step) % device_total
        pltpu.make_async_remote_copy(
            src_ref=my_hist,
            dst_ref=hists.at[me],
            send_sem=hist_send,
            recv_sem=hist_recv,
            device_id=(other // shards, other % shards),
            device_id_type=MESH,
        ).start()
        return carry

    lax.fori_loop(1, device_total, send_hist, 0)

    for i in range(6):
        receivers[i] = jnp.broadcast_to(node_rows[i], (8, nodes))
    tile_slots = TILE // source_tiles
    node = lax.broadcasted_iota(jnp.int32, (1, nodes), 1)
    link = jnp.zeros((1, nodes), jnp.int32)
    for j in range(1, shards):
        link += jnp.where(node >= j * per_peer, 1, 0)
    spot = k * per_peer + node - link * per_peer
    tile_of = jnp.zeros((1, nodes), jnp.int32)
    for t in range(1, chunks):
        tile_of += jnp.where(spot >= t * TILE, 1, 0)
    node_key = tile_of * shards + link
    where_rows = []
    for t in range(tile_slots):
        row = lax.broadcasted_iota(jnp.int32, (device_total, nodes), 0)
        key = t * shards + row % shards
        where_rows.append(jnp.where(key == node_key, 1.0, 0.0))
    place[...] = jnp.concatenate(where_rows, axis=0).astype(BF16)

    for m in range(tiles_here):
        owner = (groups * m + g) // per_shard

        @pl.when(k != owner)
        def _():
            pltpu.make_async_remote_copy(
                src_ref=packs.at[0],
                dst_ref=sources.at[m],
                send_sem=src_send.at[0],
                recv_sem=src_recv.at[m],
                device_id=(g, owner),
                device_id_type=MESH,
            ).wait_recv()

        padded = jnp.concatenate([sources[m], jnp.zeros((16 - ROWS, TILE), F32)], axis=0)
        columns[...] = jnp.transpose(padded)

        def add_sources(step, totals):
            block = columns[pl.ds(pl.multiple_of(step * 8, 8), 8), :]
            y0, y1, y2, m0, m1, m2, a, w0, w1, w2 = [
                jnp.broadcast_to(block[:, i : i + 1], (8, TILE)) for i in range(ROWS)
            ]
            result = []
            for chunk in range(chunks):
                x0, x1, x2, n0, n1, n2 = [
                    receivers[i, :, chunk * TILE : (chunk + 1) * TILE] for i in range(6)
                ]
                d0, d1, d2 = y0 - x0, y1 - x1, y2 - x2
                r2 = d0 * d0 + d1 * d1 + d2 * d2
                toward = jnp.maximum(n0 * d0 + n1 * d1 + n2 * d2, 0.0)
                facing = jnp.minimum(m0 * d0 + m1 * d1 + m2 * d2, 0.0)
                form = toward * facing / ((r2 + a) * (jnp.pi * r2 + a))
                old = totals[3 * chunk : 3 * chunk + 3]
                result += [old[0] - form * w0, old[1] - form * w1, old[2] - form * w2]
            return tuple(result)

        zero = jnp.zeros((8, TILE), F32)
        totals = lax.fori_loop(0, TILE // 8, add_sources, (zero,) * (3 * chunks), unroll=2)
        for chunk in range(chunks):
            for c in range(3):
                sums[3 * m + c : 3 * m + c + 1, chunk * TILE : (chunk + 1) * TILE] = jnp.sum(
                    totals[3 * chunk + c], axis=0, keepdims=True
                )

    all_but_one = hists.at[pl.ds(0, device_total - 1)]
    pltpu.make_async_copy(all_but_one, all_but_one, hist_recv).wait()
    table = jnp.concatenate([hists[d] for d in range(device_total)], axis=0)
    lanes = lax.broadcasted_iota(jnp.int32, (device_total, TILE), 1)
    by_tile = jnp.concatenate(
        [
            jnp.where((lanes >= t * source_tiles) & (lanes < (t + 1) * source_tiles), table, 0.0)
            for t in range(tile_slots)
        ],
        axis=0,
    ).astype(BF16)
    pick_row = lax.broadcasted_iota(jnp.int32, (16, TILE), 0)
    pick_lane = lax.broadcasted_iota(jnp.int32, (16, TILE), 1)
    pick = (pick_lane % source_tiles == groups * pick_row + g) & (pick_row < tiles_here)
    picked = lax.dot_general(
        jnp.where(pick, 1.0, 0.0).astype(BF16), by_tile, NT_DIMS, preferred_element_type=F32
    )
    weight = jnp.dot(picked.astype(BF16), place[...], preferred_element_type=F32)

    irradiance = weight[0:1] * sums[0:3, :]
    for m in range(1, tiles_here):
        irradiance += weight[m : m + 1] * sums[3 * m : 3 * m + 3, :]
    pushed = unstack3(
        jnp.dot(stack3(irradiance[:, leaves:]), onehot[...], preferred_element_type=F32), 3
    )
    part[...] = irradiance[:, :leaves] + pushed
    gathered[g] = irradiance[:, :leaves] + pushed

    def part_copy(step):
        return pltpu.make_async_remote_copy(
            src_ref=part,
            dst_ref=gathered.at[g],
            send_sem=part_send.at[step],
            recv_sem=part_recv.at[g],
            device_id=((g + step) % groups, k),
            device_id_type=MESH,
        )

    for step in range(1, groups):
        part_copy(step).start()
    for step in range(1, groups):
        sender = (g + step) % groups
        pltpu.make_async_remote_copy(
            src_ref=part,
            dst_ref=gathered.at[sender],
            send_sem=part_send.at[step],
            recv_sem=part_recv.at[sender],
            device_id=(sender, k),
            device_id_type=MESH,
        ).wait_recv()
    total = gathered[0]
    for other in range(1, groups):
        total += gathered[other]
    out[...] = total
    for step in range(1, groups):
        part_copy(step).wait_send()
    pltpu.make_async_copy(all_but_one, all_but_one, hist_send).wait()

    @pl.when(is_owner)
    def _():
        for step in range(1, shards):
            source_copy(step).wait_send()


def dense_body(
    groups, shards, leaf_emit, leaf_albedo, leaf_radiosity, leaf_area, parent_index,
    node_position, node_angles, block_receiver, block_source, block_count,
):
    leaves = leaf_area.shape[0]
    nodes = node_position.shape[1]
    clusters = nodes - leaves
    tiles_here = shards * clusters // TILE // groups
    vmem = pl.BlockSpec(memory_space=pltpu.VMEM)
    gathered = pl.pallas_call(
        functools.partial(dense_kernel, groups, shards),
        out_shape=jax.ShapeDtypeStruct((3, leaves), F32),
        in_specs=[vmem] * 7 + [pl.BlockSpec(memory_space=pltpu.SMEM)],
        out_specs=vmem,
        scratch_shapes=[
            pltpu.VMEM((clusters // TILE, ROWS, TILE), F32),
            pltpu.VMEM((tiles_here, ROWS, TILE), F32),
            pltpu.VMEM((TILE, 16), F32),
            pltpu.VMEM((1, TILE), F32),
            pltpu.VMEM((groups * shards, 1, TILE), F32),
            pltpu.VMEM((6, 8, nodes), F32),
            pltpu.VMEM((clusters, leaves), BF16),
            pltpu.VMEM((TILE // (shards * clusters // TILE) * groups * shards, nodes), BF16),
            pltpu.VMEM((3 * tiles_here, nodes), F32),
            pltpu.VMEM((3, leaves), F32),
            pltpu.VMEM((groups, 3, leaves), F32),
            pltpu.SemaphoreType.DMA((shards - 1,)),
            pltpu.SemaphoreType.DMA((tiles_here,)),
            pltpu.SemaphoreType.DMA,
            pltpu.SemaphoreType.DMA,
            pltpu.SemaphoreType.DMA((groups,)),
            pltpu.SemaphoreType.DMA((groups,)),
        ],
        compiler_params=pltpu.CompilerParams(collective_id=0, has_side_effects=True),
    )(
        leaf_radiosity, leaf_area[None, :], parent_index[None, :], node_position, node_angles,
        block_receiver, block_source, block_count,
    )
    return leaf_emit + leaf_albedo * gathered


def body(groups, shards, *args):
    leaves, nodes, slots = args[3].shape[0], args[5].shape[1], args[7].shape[1]
    per_shard = (nodes - leaves) // TILE
    source_tiles = shards * per_shard
    dense = (
        nodes // TILE * source_tiles <= TILE
        and TILE % source_tiles == 0
        and source_tiles % groups == 0
        and per_shard <= groups
        and slots == TILE
    )
    return dense_body(groups, shards, *args) if dense else listed_body(*args)


def solution(mesh):
    in_specs = (
        P(None, "dev"),
        P(None, "dev"),
        P(None, "dev"),
        P("dev"),
        P("dev"),
        P(None, "dev"),
        P(None, "dev"),
        P("grp", "dev"),
        P("grp", "dev"),
        P("grp", "dev"),
    )
    out_specs = P(None, "dev")
    sized = functools.partial(body, mesh.shape["grp"], mesh.shape["dev"])
    return jax.shard_map(sized, mesh=mesh, in_specs=in_specs, out_specs=out_specs, check_vma=False)
```

```python
import functools
import jax
import jax.numpy as jnp
from jax import lax
from jax.experimental import pallas as pl
from jax.experimental.pallas import tpu as pltpu
from jax.sharding import PartitionSpec as P

TILE = 128


batch_slots = 16


def unit_normals(node_angles):
    azimuth = node_angles[0]
    elevation = node_angles[1]
    return jnp.stack(
        [
            jnp.cos(azimuth) * jnp.cos(elevation),
            jnp.sin(azimuth) * jnp.cos(elevation),
            jnp.sin(elevation),
        ]
    )


def tile_irradiance(receivers, sources):
    offsets = [
        sources[axis_id][:, None, :] - receivers[axis_id][:, :, None] for axis_id in range(3)
    ]
    distance_sq = offsets[0] * offsets[0] + offsets[1] * offsets[1] + offsets[2] * offsets[2]
    facing_receiver = (
        receivers[3][:, :, None] * offsets[0]
        + receivers[4][:, :, None] * offsets[1]
        + receivers[5][:, :, None] * offsets[2]
    )
    facing_source = (
        sources[3][:, None, :] * offsets[0]
        + sources[4][:, None, :] * offsets[1]
        + sources[5][:, None, :] * offsets[2]
    )
    source_area = sources[6][:, None, :]
    factor = (
        source_area
        * jnp.maximum(facing_receiver, 0.0)
        * jnp.maximum(-facing_source, 0.0)
        / ((distance_sq + source_area) * (jnp.pi * distance_sq + source_area))
    )
    return jnp.einsum("bij,cbj->bci", factor, sources[7:10], precision=lax.Precision.HIGHEST)


def listed_body(
    leaf_emit,
    leaf_albedo,
    leaf_radiosity,
    leaf_area,
    parent_index,
    node_position,
    node_angles,
    block_receiver,
    block_source,
    block_count,
):
    leaf_count = leaf_area.shape[0]
    node_count = node_position.shape[1]
    cluster_count = node_count - leaf_count
    tile_count = node_count // TILE
    slot_count = block_receiver.shape[1]
    normals = unit_normals(node_angles)
    parent_onehot = (
        parent_index[:, None] == jnp.arange(cluster_count, dtype=jnp.int32)[None, :]
    ).astype(jnp.float32)
    cluster_area = jnp.dot(leaf_area, parent_onehot, precision=lax.Precision.HIGHEST)
    weighted = jnp.dot(
        leaf_radiosity * leaf_area[None, :], parent_onehot, precision=lax.Precision.HIGHEST
    )
    cluster_radiosity = weighted / cluster_area[None, :]
    source_pack = jnp.concatenate(
        [
            node_position[:, leaf_count:],
            normals[:, leaf_count:],
            cluster_area[None, :],
            cluster_radiosity,
        ],
        axis=0,
    )
    receiver_pack = jnp.concatenate([node_position, normals], axis=0)
    linked = lax.all_to_all(receiver_pack, "dev", split_axis=1, concat_axis=1, tiled=True)
    receiver_tiles = linked.reshape(6, tile_count, TILE)
    everything = lax.all_gather(source_pack, "dev", axis=1, tiled=True)
    source_tiles = everything.reshape(10, -1, TILE)
    receiver_ids = block_receiver[0]
    source_ids = block_source[0]
    live_count = block_count[0, 0]
    step_slots = min(batch_slots, slot_count)

    def add_batch(rounds, totals):
        first = rounds * step_slots
        batch_receivers = lax.dynamic_slice_in_dim(receiver_ids, first, step_slots, 0)
        batch_sources = lax.dynamic_slice_in_dim(source_ids, first, step_slots, 0)
        batch_weight = (first + jnp.arange(step_slots, dtype=jnp.int32) < live_count).astype(
            jnp.float32
        )
        receivers = jnp.take(receiver_tiles, batch_receivers, axis=1)
        sources = jnp.take(source_tiles, batch_sources, axis=1)
        contrib = tile_irradiance(receivers, sources) * batch_weight[:, None, None]
        placement = (
            batch_receivers[:, None] == jnp.arange(tile_count, dtype=jnp.int32)[None, :]
        ).astype(jnp.float32)
        return totals + jnp.einsum(
            "bt,bci->cti", placement, contrib, precision=lax.Precision.HIGHEST
        )

    batch_total = (live_count + step_slots - 1) // step_slots
    totals = lax.fori_loop(0, batch_total, add_batch, jnp.zeros((3, tile_count, TILE), jnp.float32))
    partial_value = totals.reshape(3, node_count)
    summed = lax.psum(partial_value, "grp")
    irradiance = lax.all_to_all(summed, "dev", split_axis=1, concat_axis=1, tiled=True)
    pushed = jnp.dot(irradiance[:, leaf_count:], parent_onehot.T, precision=lax.Precision.HIGHEST)
    gathered = irradiance[:, :leaf_count] + pushed
    return leaf_emit + leaf_albedo * gathered


F32 = jnp.float32
BF16 = jnp.bfloat16
MESH = pl.DeviceIdType.MESH
ROWS = 10
NT_DIMS = (((1,), (1,)), ((), ()))


def split3(values):
    high = values.astype(BF16)
    rest = values - high.astype(F32)
    middle = rest.astype(BF16)
    low = (rest - middle.astype(F32)).astype(BF16)
    return [high.astype(F32), middle.astype(F32), low.astype(F32)]


def stack3(values):
    rows = values.shape[0]
    pad = jnp.zeros((16 - 3 * rows, values.shape[1]), F32)
    return jnp.concatenate(split3(values) + [pad], axis=0).astype(BF16)


def unstack3(product, rows):
    return product[0:rows] + product[rows : 2 * rows] + product[2 * rows : 3 * rows]


def dense_kernel(
    groups, shards, *refs
):
    operands, out, inputs, scratch = refs[:8], refs[8], refs[9:17], refs[17:]
    radiosity, area, parent, position, angles, receiver_id, source_id, count = inputs
    (
        packs, sources, columns, my_hist, hists, receivers, onehot, place, sums, part, gathered,
        load, src_send, src_recv, hist_send, hist_recv, part_send, part_recv,
    ) = scratch
    g = lax.axis_index("grp")
    k = lax.axis_index("dev")
    device_total = groups * shards
    me = g * shards + k
    leaves = radiosity.shape[1]
    nodes = position.shape[1]
    clusters = nodes - leaves
    per_shard = clusters // TILE
    source_tiles = shards * per_shard
    tiles_here = source_tiles // groups
    per_peer = nodes // shards
    chunks = nodes // TILE

    barrier = pltpu.get_barrier_semaphore()

    far_first = sorted(range(shards), key=lambda step: -min(step, shards - step))
    others = [
        ((g + group_step) % groups, (k + step) % shards)
        for step in far_first
        for group_step in reversed(range(groups))
        if group_step or step
    ]
    for other in others:
        pl.semaphore_signal(barrier, inc=1, device_id=other, device_id_type=MESH)
    loads = [
        pltpu.make_async_copy(operands[i], inputs[i], load.at[i]) for i in range(len(inputs))
    ]
    for copy in loads:
        copy.start()
    for copy in loads:
        copy.wait()

    lane = lax.broadcasted_iota(jnp.int32, (1, TILE), 1)
    code = receiver_id[...] * source_tiles + source_id[...]
    code = jnp.where(lane < jnp.broadcast_to(count[...], (1, TILE)), code, -1)
    square = lax.broadcasted_iota(jnp.int32, (TILE, TILE), 0)
    hit = jnp.where(square == code, 1.0, 0.0).astype(BF16)
    counted = lax.dot_general(
        jnp.ones((16, TILE), BF16), hit, NT_DIMS, preferred_element_type=F32
    )
    my_hist[...] = counted[0:1]
    hists[me] = counted[0:1]

    ids = lax.broadcasted_iota(jnp.int32, (clusters, leaves), 0)
    onehot[...] = jnp.where(ids == parent[...], 1.0, 0.0).astype(BF16)
    area_row = area[...]
    stacked = stack3(jnp.concatenate([area_row, radiosity[...] * area_row], axis=0))
    cluster = unstack3(
        lax.dot_general(stacked, onehot[...], NT_DIMS, preferred_element_type=F32), 4
    )
    cosines = jnp.cos(angles[...])
    sines = jnp.sin(angles[...])
    normals = [cosines[0:1] * cosines[1:2], sines[0:1] * cosines[1:2], sines[1:2]]
    node_rows = [position[i : i + 1, :] for i in range(3)] + normals
    for half in range(per_shard):
        first = leaves + half * TILE
        rows = [row[:, first : first + TILE] for row in node_rows]
        rows.append(cluster[:, half * TILE : (half + 1) * TILE])
        packs[half] = jnp.concatenate(rows, axis=0)

    half = (g + groups * shards * per_shard - per_shard * k) % groups
    is_owner = half < per_shard
    mine = (per_shard * k + half) // groups

    pl.semaphore_wait(barrier, device_total - 1)

    def source_copy(step):
        return pltpu.make_async_remote_copy(
            src_ref=packs.at[half],
            dst_ref=sources.at[mine],
            send_sem=src_send.at[step - 1],
            recv_sem=src_recv.at[mine],
            device_id=(g, (k + step) % shards),
            device_id_type=MESH,
        )

    @pl.when(is_owner)
    def _():
        for step in range(1, shards):
            source_copy(step).start()
        sources[mine] = packs[half]

    for other in others:
        pltpu.make_async_remote_copy(
            src_ref=my_hist,
            dst_ref=hists.at[me],
            send_sem=hist_send,
            recv_sem=hist_recv,
            device_id=other,
            device_id_type=MESH,
        ).start()

    for i in range(6):
        receivers[i] = jnp.broadcast_to(node_rows[i], (8, nodes))
    tile_slots = TILE // source_tiles
    node = lax.broadcasted_iota(jnp.int32, (1, nodes), 1)
    link = jnp.zeros((1, nodes), jnp.int32)
    for j in range(1, shards):
        link += jnp.where(node >= j * per_peer, 1, 0)
    spot = k * per_peer + node - link * per_peer
    tile_of = jnp.zeros((1, nodes), jnp.int32)
    for t in range(1, chunks):
        tile_of += jnp.where(spot >= t * TILE, 1, 0)
    node_key = tile_of * shards + link
    where_rows = []
    for t in range(tile_slots):
        row = lax.broadcasted_iota(jnp.int32, (device_total, nodes), 0)
        key = t * shards + row % shards
        where_rows.append(jnp.where(key == node_key, 1.0, 0.0))
    place[...] = jnp.concatenate(where_rows, axis=0).astype(BF16)

    for m in range(tiles_here):
        owner = (groups * m + g) // per_shard

        @pl.when(k != owner)
        def _():
            pltpu.make_async_remote_copy(
                src_ref=packs.at[0],
                dst_ref=sources.at[m],
                send_sem=src_send.at[0],
                recv_sem=src_recv.at[m],
                device_id=(g, owner),
                device_id_type=MESH,
            ).wait_recv()

        padded = jnp.concatenate([sources[m], jnp.zeros((16 - ROWS, TILE), F32)], axis=0)
        columns[...] = jnp.transpose(padded)

        def add_sources(step, totals):
            block = columns[pl.ds(pl.multiple_of(step * 8, 8), 8), :]
            y0, y1, y2, m0, m1, m2, a, w0, w1, w2 = [
                jnp.broadcast_to(block[:, i : i + 1], (8, TILE)) for i in range(ROWS)
            ]
            result = []
            for chunk in range(chunks):
                x0, x1, x2, n0, n1, n2 = [
                    receivers[i, :, chunk * TILE : (chunk + 1) * TILE] for i in range(6)
                ]
                d0, d1, d2 = y0 - x0, y1 - x1, y2 - x2
                r2 = d0 * d0 + d1 * d1 + d2 * d2
                toward = jnp.maximum(n0 * d0 + n1 * d1 + n2 * d2, 0.0)
                facing = jnp.minimum(m0 * d0 + m1 * d1 + m2 * d2, 0.0)
                form = toward * facing / ((r2 + a) * (jnp.pi * r2 + a))
                old = totals[3 * chunk : 3 * chunk + 3]
                result += [old[0] - form * w0, old[1] - form * w1, old[2] - form * w2]
            return tuple(result)

        zero = jnp.zeros((8, TILE), F32)
        totals = lax.fori_loop(0, TILE // 8, add_sources, (zero,) * (3 * chunks), unroll=8)
        for chunk in range(chunks):
            for c in range(3):
                sums[3 * m + c : 3 * m + c + 1, chunk * TILE : (chunk + 1) * TILE] = jnp.sum(
                    totals[3 * chunk + c], axis=0, keepdims=True
                )

    all_but_one = hists.at[pl.ds(0, device_total - 1)]
    pltpu.make_async_copy(all_but_one, all_but_one, hist_recv).wait()
    table = jnp.concatenate([hists[d] for d in range(device_total)], axis=0)
    lanes = lax.broadcasted_iota(jnp.int32, (device_total, TILE), 1)
    by_tile = jnp.concatenate(
        [
            jnp.where((lanes >= t * source_tiles) & (lanes < (t + 1) * source_tiles), table, 0.0)
            for t in range(tile_slots)
        ],
        axis=0,
    ).astype(BF16)
    pick_row = lax.broadcasted_iota(jnp.int32, (16, TILE), 0)
    pick_lane = lax.broadcasted_iota(jnp.int32, (16, TILE), 1)
    pick = (pick_lane % source_tiles == groups * pick_row + g) & (pick_row < tiles_here)
    picked = lax.dot_general(
        jnp.where(pick, 1.0, 0.0).astype(BF16), by_tile, NT_DIMS, preferred_element_type=F32
    )
    weight = jnp.dot(picked.astype(BF16), place[...], preferred_element_type=F32)

    irradiance = weight[0:1] * sums[0:3, :]
    for m in range(1, tiles_here):
        irradiance += weight[m : m + 1] * sums[3 * m : 3 * m + 3, :]
    pushed = unstack3(
        jnp.dot(stack3(irradiance[:, leaves:]), onehot[...], preferred_element_type=F32), 3
    )
    part[...] = irradiance[:, :leaves] + pushed
    gathered[g] = irradiance[:, :leaves] + pushed

    def part_copy(step):
        return pltpu.make_async_remote_copy(
            src_ref=part,
            dst_ref=gathered.at[g],
            send_sem=part_send.at[step],
            recv_sem=part_recv.at[g],
            device_id=((g + step) % groups, k),
            device_id_type=MESH,
        )

    for step in range(1, groups):
        part_copy(step).start()
    for step in range(1, groups):
        sender = (g + step) % groups
        pltpu.make_async_remote_copy(
            src_ref=part,
            dst_ref=gathered.at[sender],
            send_sem=part_send.at[step],
            recv_sem=part_recv.at[sender],
            device_id=(sender, k),
            device_id_type=MESH,
        ).wait_recv()
    total = gathered[0]
    for other in range(1, groups):
        total += gathered[other]
    out[...] = total
    for step in range(1, groups):
        part_copy(step).wait_send()
    pltpu.make_async_copy(all_but_one, all_but_one, hist_send).wait()

    @pl.when(is_owner)
    def _():
        for step in range(1, shards):
            source_copy(step).wait_send()


def dense_body(
    groups, shards, leaf_emit, leaf_albedo, leaf_radiosity, leaf_area, parent_index,
    node_position, node_angles, block_receiver, block_source, block_count,
):
    leaves = leaf_area.shape[0]
    nodes = node_position.shape[1]
    clusters = nodes - leaves
    tiles_here = shards * clusters // TILE // groups
    operands = (
        leaf_radiosity, leaf_area[None, :], parent_index[None, :], node_position, node_angles,
        block_receiver, block_source, block_count,
    )
    gathered = pl.pallas_call(
        functools.partial(dense_kernel, groups, shards),
        out_shape=pltpu.VMEM((3, leaves), F32),
        in_specs=[pl.BlockSpec(memory_space=pl.ANY)] * len(operands),
        out_specs=pl.BlockSpec(memory_space=pltpu.VMEM),
        scratch_shapes=[pltpu.VMEM(x.shape, x.dtype) for x in operands]
        + [
            pltpu.VMEM((clusters // TILE, ROWS, TILE), F32),
            pltpu.VMEM((tiles_here, ROWS, TILE), F32),
            pltpu.VMEM((TILE, 16), F32),
            pltpu.VMEM((1, TILE), F32),
            pltpu.VMEM((groups * shards, 1, TILE), F32),
            pltpu.VMEM((6, 8, nodes), F32),
            pltpu.VMEM((clusters, leaves), BF16),
            pltpu.VMEM((TILE // (shards * clusters // TILE) * groups * shards, nodes), BF16),
            pltpu.VMEM((3 * tiles_here, nodes), F32),
            pltpu.VMEM((3, leaves), F32),
            pltpu.VMEM((groups, 3, leaves), F32),
            pltpu.SemaphoreType.DMA((len(operands),)),
            pltpu.SemaphoreType.DMA((shards - 1,)),
            pltpu.SemaphoreType.DMA((tiles_here,)),
            pltpu.SemaphoreType.DMA,
            pltpu.SemaphoreType.DMA,
            pltpu.SemaphoreType.DMA((groups,)),
            pltpu.SemaphoreType.DMA((groups,)),
        ],
        compiler_params=pltpu.CompilerParams(collective_id=0, has_side_effects=True),
    )(*operands)
    return leaf_emit + leaf_albedo * gathered


def body(groups, shards, *args):
    leaves, nodes, slots = args[3].shape[0], args[5].shape[1], args[7].shape[1]
    per_shard = (nodes - leaves) // TILE
    source_tiles = shards * per_shard
    dense = (
        nodes // TILE * source_tiles <= TILE
        and TILE % source_tiles == 0
        and source_tiles % groups == 0
        and per_shard <= groups
        and slots == TILE
    )
    return dense_body(groups, shards, *args) if dense else listed_body(*args)


def solution(mesh):
    in_specs = (
        P(None, "dev"),
        P(None, "dev"),
        P(None, "dev"),
        P("dev"),
        P("dev"),
        P(None, "dev"),
        P(None, "dev"),
        P("grp", "dev"),
        P("grp", "dev"),
        P("grp", "dev"),
    )
    out_specs = P(None, "dev")
    sized = functools.partial(body, mesh.shape["grp"], mesh.shape["dev"])
    return jax.shard_map(sized, mesh=mesh, in_specs=in_specs, out_specs=out_specs, check_vma=False)
```

```python
import functools
import jax
import jax.numpy as jnp
from jax import lax
from jax.experimental import pallas as pl
from jax.experimental.pallas import tpu as pltpu
from jax.sharding import PartitionSpec as P

TILE = 128


batch_slots = 16


def unit_normals(node_angles):
    azimuth = node_angles[0]
    elevation = node_angles[1]
    return jnp.stack(
        [
            jnp.cos(azimuth) * jnp.cos(elevation),
            jnp.sin(azimuth) * jnp.cos(elevation),
            jnp.sin(elevation),
        ]
    )


def tile_irradiance(receivers, sources):
    offsets = [
        sources[axis_id][:, None, :] - receivers[axis_id][:, :, None] for axis_id in range(3)
    ]
    distance_sq = offsets[0] * offsets[0] + offsets[1] * offsets[1] + offsets[2] * offsets[2]
    facing_receiver = (
        receivers[3][:, :, None] * offsets[0]
        + receivers[4][:, :, None] * offsets[1]
        + receivers[5][:, :, None] * offsets[2]
    )
    facing_source = (
        sources[3][:, None, :] * offsets[0]
        + sources[4][:, None, :] * offsets[1]
        + sources[5][:, None, :] * offsets[2]
    )
    source_area = sources[6][:, None, :]
    factor = (
        source_area
        * jnp.maximum(facing_receiver, 0.0)
        * jnp.maximum(-facing_source, 0.0)
        / ((distance_sq + source_area) * (jnp.pi * distance_sq + source_area))
    )
    return jnp.einsum("bij,cbj->bci", factor, sources[7:10], precision=lax.Precision.HIGHEST)


def listed_body(
    leaf_emit,
    leaf_albedo,
    leaf_radiosity,
    leaf_area,
    parent_index,
    node_position,
    node_angles,
    block_receiver,
    block_source,
    block_count,
):
    leaf_count = leaf_area.shape[0]
    node_count = node_position.shape[1]
    cluster_count = node_count - leaf_count
    tile_count = node_count // TILE
    slot_count = block_receiver.shape[1]
    normals = unit_normals(node_angles)
    parent_onehot = (
        parent_index[:, None] == jnp.arange(cluster_count, dtype=jnp.int32)[None, :]
    ).astype(jnp.float32)
    cluster_area = jnp.dot(leaf_area, parent_onehot, precision=lax.Precision.HIGHEST)
    weighted = jnp.dot(
        leaf_radiosity * leaf_area[None, :], parent_onehot, precision=lax.Precision.HIGHEST
    )
    cluster_radiosity = weighted / cluster_area[None, :]
    source_pack = jnp.concatenate(
        [
            node_position[:, leaf_count:],
            normals[:, leaf_count:],
            cluster_area[None, :],
            cluster_radiosity,
        ],
        axis=0,
    )
    receiver_pack = jnp.concatenate([node_position, normals], axis=0)
    linked = lax.all_to_all(receiver_pack, "dev", split_axis=1, concat_axis=1, tiled=True)
    receiver_tiles = linked.reshape(6, tile_count, TILE)
    everything = lax.all_gather(source_pack, "dev", axis=1, tiled=True)
    source_tiles = everything.reshape(10, -1, TILE)
    receiver_ids = block_receiver[0]
    source_ids = block_source[0]
    live_count = block_count[0, 0]
    step_slots = min(batch_slots, slot_count)

    def add_batch(rounds, totals):
        first = rounds * step_slots
        batch_receivers = lax.dynamic_slice_in_dim(receiver_ids, first, step_slots, 0)
        batch_sources = lax.dynamic_slice_in_dim(source_ids, first, step_slots, 0)
        batch_weight = (first + jnp.arange(step_slots, dtype=jnp.int32) < live_count).astype(
            jnp.float32
        )
        receivers = jnp.take(receiver_tiles, batch_receivers, axis=1)
        sources = jnp.take(source_tiles, batch_sources, axis=1)
        contrib = tile_irradiance(receivers, sources) * batch_weight[:, None, None]
        placement = (
            batch_receivers[:, None] == jnp.arange(tile_count, dtype=jnp.int32)[None, :]
        ).astype(jnp.float32)
        return totals + jnp.einsum(
            "bt,bci->cti", placement, contrib, precision=lax.Precision.HIGHEST
        )

    batch_total = (live_count + step_slots - 1) // step_slots
    totals = lax.fori_loop(0, batch_total, add_batch, jnp.zeros((3, tile_count, TILE), jnp.float32))
    partial_value = totals.reshape(3, node_count)
    summed = lax.psum(partial_value, "grp")
    irradiance = lax.all_to_all(summed, "dev", split_axis=1, concat_axis=1, tiled=True)
    pushed = jnp.dot(irradiance[:, leaf_count:], parent_onehot.T, precision=lax.Precision.HIGHEST)
    gathered = irradiance[:, :leaf_count] + pushed
    return leaf_emit + leaf_albedo * gathered


F32 = jnp.float32
BF16 = jnp.bfloat16
MESH = pl.DeviceIdType.MESH
ROWS = 10
NT_DIMS = (((1,), (1,)), ((), ()))


def split3(values):
    high = values.astype(BF16)
    rest = values - high.astype(F32)
    middle = rest.astype(BF16)
    low = (rest - middle.astype(F32)).astype(BF16)
    return [high.astype(F32), middle.astype(F32), low.astype(F32)]


def stack3(values):
    rows = values.shape[0]
    pad = jnp.zeros((16 - 3 * rows, values.shape[1]), F32)
    return jnp.concatenate(split3(values) + [pad], axis=0).astype(BF16)


def unstack3(product, rows):
    return product[0:rows] + product[rows : 2 * rows] + product[2 * rows : 3 * rows]


def dense_kernel(
    groups, shards, *refs
):
    operands, out, inputs, scratch = refs[:8], refs[8], refs[9:17], refs[17:]
    radiosity, area, parent, position, angles, receiver_id, source_id, count = inputs
    (
        packs, sources, columns, my_hist, hists, receivers, onehot, place, sums, part, gathered,
        load, src_send, src_recv, hist_send, hist_recv, part_send, part_recv,
    ) = scratch
    g = lax.axis_index("grp")
    k = lax.axis_index("dev")
    device_total = groups * shards
    me = g * shards + k
    leaves = radiosity.shape[1]
    nodes = position.shape[1]
    clusters = nodes - leaves
    per_shard = clusters // TILE
    source_tiles = shards * per_shard
    tiles_here = source_tiles // groups
    per_peer = nodes // shards
    chunks = nodes // TILE

    barrier = pltpu.get_barrier_semaphore()

    far_first = sorted(range(shards), key=lambda step: -min(step, shards - step))
    others = [
        ((g + group_step) % groups, (k + step) % shards)
        for step in far_first
        for group_step in reversed(range(groups))
        if group_step or step
    ]
    for other in others:
        pl.semaphore_signal(barrier, inc=1, device_id=other, device_id_type=MESH)
    loads = [
        pltpu.make_async_copy(operands[i], inputs[i], load.at[i]) for i in range(len(inputs))
    ]
    for copy in loads:
        copy.start()
    for copy in loads:
        copy.wait()

    lane = lax.broadcasted_iota(jnp.int32, (1, TILE), 1)
    code = receiver_id[...] * source_tiles + source_id[...]
    code = jnp.where(lane < jnp.broadcast_to(count[...], (1, TILE)), code, -1)
    square = lax.broadcasted_iota(jnp.int32, (TILE, TILE), 0)
    hit = jnp.where(square == code, 1.0, 0.0).astype(BF16)
    counted = lax.dot_general(
        jnp.ones((16, TILE), BF16), hit, NT_DIMS, preferred_element_type=F32
    )
    my_hist[...] = counted[0:1]
    hists[me] = counted[0:1]

    ids = lax.broadcasted_iota(jnp.int32, (clusters, leaves), 0)
    onehot[...] = jnp.where(ids == parent[...], 1.0, 0.0).astype(BF16)
    area_row = area[...]
    stacked = stack3(jnp.concatenate([area_row, radiosity[...] * area_row], axis=0))
    cluster = unstack3(
        lax.dot_general(stacked, onehot[...], NT_DIMS, preferred_element_type=F32), 4
    )
    cosines = jnp.cos(angles[...])
    sines = jnp.sin(angles[...])
    normals = [cosines[0:1] * cosines[1:2], sines[0:1] * cosines[1:2], sines[1:2]]
    node_rows = [position[i : i + 1, :] for i in range(3)] + normals
    for half in range(per_shard):
        first = leaves + half * TILE
        rows = [row[:, first : first + TILE] for row in node_rows]
        rows.append(cluster[:, half * TILE : (half + 1) * TILE])
        packs[half] = jnp.concatenate(rows, axis=0)

    half = (g + groups * shards * per_shard - per_shard * k) % groups
    is_owner = half < per_shard
    mine = (per_shard * k + half) // groups

    pl.semaphore_wait(barrier, device_total - 1)

    def source_copy(step):
        return pltpu.make_async_remote_copy(
            src_ref=packs.at[half],
            dst_ref=sources.at[mine],
            send_sem=src_send.at[step - 1],
            recv_sem=src_recv.at[mine],
            device_id=(g, (k + step) % shards),
            device_id_type=MESH,
        )

    @pl.when(is_owner)
    def _():
        for step in range(1, shards):
            source_copy(step).start()
        sources[mine] = packs[half]

    for other in others:
        pltpu.make_async_remote_copy(
            src_ref=my_hist,
            dst_ref=hists.at[me],
            send_sem=hist_send,
            recv_sem=hist_recv,
            device_id=other,
            device_id_type=MESH,
        ).start()

    for i in range(6):
        receivers[i] = jnp.broadcast_to(node_rows[i], (8, nodes))
    tile_slots = TILE // source_tiles
    node = lax.broadcasted_iota(jnp.int32, (1, nodes), 1)
    link = jnp.zeros((1, nodes), jnp.int32)
    for j in range(1, shards):
        link += jnp.where(node >= j * per_peer, 1, 0)
    spot = k * per_peer + node - link * per_peer
    tile_of = jnp.zeros((1, nodes), jnp.int32)
    for t in range(1, chunks):
        tile_of += jnp.where(spot >= t * TILE, 1, 0)
    node_key = tile_of * shards + link
    where_rows = []
    for t in range(tile_slots):
        row = lax.broadcasted_iota(jnp.int32, (device_total, nodes), 0)
        key = t * shards + row % shards
        where_rows.append(jnp.where(key == node_key, 1.0, 0.0))
    place[...] = jnp.concatenate(where_rows, axis=0).astype(BF16)

    nearest = per_shard * k // groups
    for turn in range(tiles_here):
        m = (nearest + turn) % tiles_here
        owner = (groups * m + g) // per_shard

        @pl.when(k != owner)
        def _():
            pltpu.make_async_remote_copy(
                src_ref=packs.at[0],
                dst_ref=sources.at[m],
                send_sem=src_send.at[0],
                recv_sem=src_recv.at[m],
                device_id=(g, owner),
                device_id_type=MESH,
            ).wait_recv()

        padded = jnp.concatenate([sources[m], jnp.zeros((16 - ROWS, TILE), F32)], axis=0)
        columns[...] = jnp.transpose(padded)

        def add_sources(step, totals):
            block = columns[pl.ds(pl.multiple_of(step * 8, 8), 8), :]
            y0, y1, y2, m0, m1, m2, a, w0, w1, w2 = [
                jnp.broadcast_to(block[:, i : i + 1], (8, TILE)) for i in range(ROWS)
            ]
            result = []
            for chunk in range(chunks):
                x0, x1, x2, n0, n1, n2 = [
                    receivers[i, :, chunk * TILE : (chunk + 1) * TILE] for i in range(6)
                ]
                d0, d1, d2 = y0 - x0, y1 - x1, y2 - x2
                r2 = d0 * d0 + d1 * d1 + d2 * d2
                toward = jnp.maximum(n0 * d0 + n1 * d1 + n2 * d2, 0.0)
                facing = jnp.minimum(m0 * d0 + m1 * d1 + m2 * d2, 0.0)
                form = toward * facing / ((r2 + a) * (jnp.pi * r2 + a))
                old = totals[3 * chunk : 3 * chunk + 3]
                result += [old[0] - form * w0, old[1] - form * w1, old[2] - form * w2]
            return tuple(result)

        zero = jnp.zeros((8, TILE), F32)
        totals = lax.fori_loop(0, TILE // 8, add_sources, (zero,) * (3 * chunks), unroll=8)
        for chunk in range(chunks):
            for c in range(3):
                sums[3 * turn + c : 3 * turn + c + 1, chunk * TILE : (chunk + 1) * TILE] = jnp.sum(
                    totals[3 * chunk + c], axis=0, keepdims=True
                )

    all_but_one = hists.at[pl.ds(0, device_total - 1)]
    pltpu.make_async_copy(all_but_one, all_but_one, hist_recv).wait()
    table = jnp.concatenate([hists[d] for d in range(device_total)], axis=0)
    lanes = lax.broadcasted_iota(jnp.int32, (device_total, TILE), 1)
    by_tile = jnp.concatenate(
        [
            jnp.where((lanes >= t * source_tiles) & (lanes < (t + 1) * source_tiles), table, 0.0)
            for t in range(tile_slots)
        ],
        axis=0,
    ).astype(BF16)
    pick_row = lax.broadcasted_iota(jnp.int32, (16, TILE), 0)
    pick_lane = lax.broadcasted_iota(jnp.int32, (16, TILE), 1)
    pick = (pick_lane % source_tiles == groups * ((nearest + pick_row) % tiles_here) + g) & (pick_row < tiles_here)
    picked = lax.dot_general(
        jnp.where(pick, 1.0, 0.0).astype(BF16), by_tile, NT_DIMS, preferred_element_type=F32
    )
    weight = jnp.dot(picked.astype(BF16), place[...], preferred_element_type=F32)

    irradiance = weight[0:1] * sums[0:3, :]
    for m in range(1, tiles_here):
        irradiance += weight[m : m + 1] * sums[3 * m : 3 * m + 3, :]
    pushed = unstack3(
        jnp.dot(stack3(irradiance[:, leaves:]), onehot[...], preferred_element_type=F32), 3
    )
    part[...] = irradiance[:, :leaves] + pushed
    gathered[g] = irradiance[:, :leaves] + pushed

    def part_copy(step):
        return pltpu.make_async_remote_copy(
            src_ref=part,
            dst_ref=gathered.at[g],
            send_sem=part_send.at[step],
            recv_sem=part_recv.at[g],
            device_id=((g + step) % groups, k),
            device_id_type=MESH,
        )

    for step in range(1, groups):
        part_copy(step).start()
    for step in range(1, groups):
        sender = (g + step) % groups
        pltpu.make_async_remote_copy(
            src_ref=part,
            dst_ref=gathered.at[sender],
            send_sem=part_send.at[step],
            recv_sem=part_recv.at[sender],
            device_id=(sender, k),
            device_id_type=MESH,
        ).wait_recv()
    total = gathered[0]
    for other in range(1, groups):
        total += gathered[other]
    out[...] = total
    for step in range(1, groups):
        part_copy(step).wait_send()
    pltpu.make_async_copy(all_but_one, all_but_one, hist_send).wait()

    @pl.when(is_owner)
    def _():
        for step in range(1, shards):
            source_copy(step).wait_send()


def dense_body(
    groups, shards, leaf_emit, leaf_albedo, leaf_radiosity, leaf_area, parent_index,
    node_position, node_angles, block_receiver, block_source, block_count,
):
    leaves = leaf_area.shape[0]
    nodes = node_position.shape[1]
    clusters = nodes - leaves
    tiles_here = shards * clusters // TILE // groups
    operands = (
        leaf_radiosity, leaf_area[None, :], parent_index[None, :], node_position, node_angles,
        block_receiver, block_source, block_count,
    )
    gathered = pl.pallas_call(
        functools.partial(dense_kernel, groups, shards),
        out_shape=pltpu.VMEM((3, leaves), F32),
        in_specs=[pl.BlockSpec(memory_space=pl.ANY)] * len(operands),
        out_specs=pl.BlockSpec(memory_space=pltpu.VMEM),
        scratch_shapes=[pltpu.VMEM(x.shape, x.dtype) for x in operands]
        + [
            pltpu.VMEM((clusters // TILE, ROWS, TILE), F32),
            pltpu.VMEM((tiles_here, ROWS, TILE), F32),
            pltpu.VMEM((TILE, 16), F32),
            pltpu.VMEM((1, TILE), F32),
            pltpu.VMEM((groups * shards, 1, TILE), F32),
            pltpu.VMEM((6, 8, nodes), F32),
            pltpu.VMEM((clusters, leaves), BF16),
            pltpu.VMEM((TILE // (shards * clusters // TILE) * groups * shards, nodes), BF16),
            pltpu.VMEM((3 * tiles_here, nodes), F32),
            pltpu.VMEM((3, leaves), F32),
            pltpu.VMEM((groups, 3, leaves), F32),
            pltpu.SemaphoreType.DMA((len(operands),)),
            pltpu.SemaphoreType.DMA((shards - 1,)),
            pltpu.SemaphoreType.DMA((tiles_here,)),
            pltpu.SemaphoreType.DMA,
            pltpu.SemaphoreType.DMA,
            pltpu.SemaphoreType.DMA((groups,)),
            pltpu.SemaphoreType.DMA((groups,)),
        ],
        compiler_params=pltpu.CompilerParams(collective_id=0, has_side_effects=True),
    )(*operands)
    return leaf_emit + leaf_albedo * gathered


def body(groups, shards, *args):
    leaves, nodes, slots = args[3].shape[0], args[5].shape[1], args[7].shape[1]
    per_shard = (nodes - leaves) // TILE
    source_tiles = shards * per_shard
    dense = (
        nodes // TILE * source_tiles <= TILE
        and TILE % source_tiles == 0
        and source_tiles % groups == 0
        and per_shard <= groups
        and slots == TILE
    )
    return dense_body(groups, shards, *args) if dense else listed_body(*args)


def solution(mesh):
    in_specs = (
        P(None, "dev"),
        P(None, "dev"),
        P(None, "dev"),
        P("dev"),
        P("dev"),
        P(None, "dev"),
        P(None, "dev"),
        P("grp", "dev"),
        P("grp", "dev"),
        P("grp", "dev"),
    )
    out_specs = P(None, "dev")
    sized = functools.partial(body, mesh.shape["grp"], mesh.shape["dev"])
    return jax.shard_map(sized, mesh=mesh, in_specs=in_specs, out_specs=out_specs, check_vma=False)
```
